32 devices in a mesh: row: 8 (over z, x), col: 2 (over y), rep: 2 (over core).
Axes of the slice: x: 2, y: 2, z: 4, core: 2. Of those that a mesh axis runs over, the one named last changes fastest.
Arguments:
- matrix: float32 [16384, 16384], P('row', 'col'), may hold values from -0.125 to 0.125
- vectors: float32 [64, 16384], P('rep', 'row'), may hold values from -0.3 to 0.3
Outputs:
- result: float32 [64, 16384], P('rep', 'row')
The draws below stay inside these ranges and needn't reach their ends.
All inputs are finite; a program needn't handle non-finite values.
Results may differ from the reference program's by a relative error of at most 0.00011.
Values sent between devices are 32-bit elements; how exact they have to be, the bound alone decides.
A program may use at most 128 MiB of HBM per device.

```python
import jax
import jax.numpy as jnp
from jax import lax

N = 16384
COLS = 64
TERMS = 6
STEPS = 1


def block_scale(rng, dims, split, smallest, largest):
    factor_of = 1.0
    for position, blocks in split:
        steps = jax.random.uniform(jax.random.fold_in(jax.random.fold_in(rng, 6), position), (blocks,), jnp.float32, smallest / len(split), largest / len(split))
        factor_of = factor_of * jnp.repeat(jnp.exp(steps), dims[position] // blocks).reshape((-1,) + (1,) * (len(dims) - 1 - position))
    return factor_of


def gaussian(stream_key, shape, deviation, limit, pieces=(), dtype=jnp.bfloat16):
    factor_of = block_scale(stream_key, shape, pieces, -0.22, 0.18) if pieces else 1.0
    entries = jax.random.normal(stream_key, shape, jnp.float32) * deviation * factor_of
    return jnp.minimum(jnp.maximum(entries, -limit), limit).astype(dtype)


def setup_inputs(seed: int = 0) -> dict:
    key_list = jax.random.split(jax.random.key(seed), 3)
    matrix = gaussian(key_list[0], (N, N), (N // 7) ** -0.5, 0.125, ((0, 8), (1, 2)), jnp.float32)
    vectors = gaussian(key_list[1], (COLS, N), 0.05, 0.3, ((0, 2), (1, 8)), jnp.float32)
    return {"matrix": matrix, "vectors": vectors}


def reference(matrix, vectors):
    current = vectors
    for section in range(STEPS):
        summand = current
        running = current
        for degree in range(1, TERMS + 1):
            product = lax.dot_general(summand, matrix, (((1,), (1,)), ((), ())), precision=lax.Precision.HIGHEST, preferred_element_type=jnp.float32)
            summand = product / float(degree * STEPS)
            running = running + summand
        current = running
    return current
```

```python
import functools

import jax
import jax.numpy as jnp
from jax import lax
from jax.experimental import pallas as pl
from jax.experimental.pallas import tpu as pltpu
from jax.sharding import PartitionSpec as P

TERMS = 6
STEPS = 1
MESH = pl.DeviceIdType.MESH
TILE = 256
SLOTS = 4


def kernel(
    rows, cols, m_ref, v_ref, out_ref,
    high, low, stage, xbuf, acc, drecv, ybuf, run, fin, frecv,
    stage_sem, init_send, init_recv, x_recv, up_send, down_send, pair_send,
    d_send, d_recv, y_send, y_recv, f_send, f_recv,
):
    fanout = rows // cols
    size = m_ref.shape[0]
    share = v_ref.shape[0]
    half = size // 2
    chunks = half // TILE
    tiles = size // TILE
    lines = rows // 2
    depth = fanout // 2
    total = fanout * chunks

    r, c, p = lax.axis_index("row"), lax.axis_index("col"), lax.axis_index("rep")
    z, x = r // 2, r % 2
    first_line = c * depth
    owner = r // fanout
    own = owner == c
    mine = r % fanout

    barrier = pltpu.get_barrier_semaphore()

    def greet(**where):
        pl.semaphore_signal(barrier, inc=1, device_id=where, device_id_type=MESH)

    greet(rep=1 - p)
    greet(row=z * 2 + 1 - x)
    for offset in range(1, cols):
        greet(col=(c + offset) % cols)

    @pl.when(z > 0)
    def _():
        greet(row=r - 2)

    @pl.when(z < lines - 1)
    def _():
        greet(row=r + 2)

    def block_of(index):
        line = jnp.where(z > first_line, depth - 1 - index // 2, index // 2)
        lane = jnp.where(index % 2 == 0, x, 1 - x)
        return line, lane, line * 2 + lane

    def load(step):
        _, _, j = block_of(step % fanout)
        start = pl.multiple_of(j * size + p * half + (step // fanout) * TILE, TILE)
        return pltpu.make_async_copy(
            m_ref.at[:, pl.ds(start, TILE)], stage.at[step % SLOTS], stage_sem.at[step % SLOTS]
        )

    for step in range(min(SLOTS, total)):
        load(step).start()

    pl.semaphore_wait(barrier, 1 + cols + (z > 0).astype(jnp.int32) + (z < lines - 1).astype(jnp.int32))

    def remote(source, target, send, recv, **where):
        return pltpu.make_async_remote_copy(
            src_ref=source, dst_ref=target, send_sem=send, recv_sem=recv,
            device_id=where, device_id_type=MESH,
        )

    def hops(s, line, lane, j, k):
        ref, recv = xbuf.at[s, j, k], x_recv.at[s % 2, j, k]
        here = lane == x
        return (
            (here & (z >= line) & (z < lines - 1), remote(ref, ref, up_send.at[j, k], recv, row=r + 2)),
            (here & (z <= line) & (z > 0), remote(ref, ref, down_send.at[j, k], recv, row=r - 2)),
            (here, remote(ref, ref, pair_send.at[j, k], recv, row=z * 2 + 1 - x)),
        )

    def pass_on(s, line, lane, j, k, again):
        for needed, copy in hops(s, line, lane, j, k):
            @pl.when(needed)
            def _(copy=copy):
                if again:
                    copy.wait_send()
                copy.start()

    def pass_own(s, k, again):
        pass_on(s, z, x, mine, k, again)

    @pl.when(own)
    def _():
        def given(k):
            start = pl.multiple_of((1 - p) * half + k * TILE, TILE)
            return remote(
                v_ref.at[:, pl.ds(start, TILE)],
                xbuf.at[0, mine, k, pl.ds(pl.multiple_of(p * share, share), share), :],
                init_send.at[k], init_recv.at[k], rep=1 - p,
            )

        for k in range(chunks):
            given(k).start()
        for k in range(chunks):
            start = pl.multiple_of(p * half + k * TILE, TILE)
            xbuf[0, mine, k, pl.ds(pl.multiple_of(p * share, share), share), :] = v_ref[:, pl.ds(start, TILE)]
        for k in range(chunks):
            given(k).wait()
            run[k] = xbuf[0, mine, k]
            pass_own(0, k, False)

    @pl.when(jnp.logical_not(own))
    def _():
        run[...] = jnp.zeros_like(run)

    def prepare(step, index):
        load(step).wait()
        for n in range(tiles):
            block = stage[step % SLOTS, n * TILE:(n + 1) * TILE, :]
            top = block.astype(jnp.bfloat16)
            rest = (block - top.astype(jnp.float32)).astype(jnp.bfloat16)
            high[index, n] = top.T
            low[index, n] = rest.T

        @pl.when(step + SLOTS < total)
        def _():
            load(step + SLOTS).start()

    def multiply(s, first):
        acc[...] = jnp.zeros_like(acc)

        def body(step, carry):
            line, lane, j = block_of(step % fanout)
            k = step // fanout
            index = j * chunks + k
            if first:
                prepare(step, index)

            @pl.when(r != c * fanout + j)
            def _():
                remote(xbuf.at[s, j, k], xbuf.at[s, j, k], up_send.at[j, k], x_recv.at[s % 2, j, k], rep=1 - p).wait_recv()
                pass_on(s, first_line + line, lane, j, k, not first)

            value = xbuf[s, j, k]
            top = value.astype(jnp.bfloat16)
            rest = (value - top.astype(jnp.float32)).astype(jnp.bfloat16)
            both = jnp.concatenate([top, rest], axis=0)
            count = value.shape[0]
            for n in range(tiles):
                large = jnp.dot(both, high[index, n], preferred_element_type=jnp.float32)
                small = jnp.dot(top, low[index, n], preferred_element_type=jnp.float32)
                acc[n] += large[:count] + (large[count:] + small)
            return carry

        lax.fori_loop(0, total, body, 0)

    def swap(s, k):
        return remote(
            acc.at[(1 - p) * chunks + k], drecv.at[s, k], d_send.at[k], d_recv.at[s % 2, k], rep=1 - p
        )

    def to_column(s, k, target):
        return remote(
            ybuf.at[s, c, k], ybuf.at[s, c, k], y_send.at[target, k], y_recv.at[s % 2, c, k], col=target
        )

    def from_column(s, k, source):
        return remote(
            ybuf.at[s, source, k], ybuf.at[s, source, k], y_send.at[source, k], y_recv.at[s % 2, source, k], col=source
        )

    def column_sum(s, k):
        for offset in range(1, cols):
            from_column(s, k, (c + offset) % cols).wait_recv()
        value = ybuf[s, 0, k]
        for source in range(1, cols):
            value = value + ybuf[s, source, k]
        return value

    def scaled(s, k):
        swap(s, k).wait_recv()
        degree = jnp.asarray((s + 1) * STEPS, jnp.int32).astype(jnp.float32)
        return (acc[p * chunks + k] + drecv[s, k]) / degree

    def reduce(s, first):
        for k in range(chunks):
            swap(s, k).start()

        @pl.when(own)
        def _():
            for k in range(chunks):
                ybuf[s, c, k] = scaled(s, k)
                value = column_sum(s, k)
                xbuf[s + 1, mine, k] = value
                run[k] = run[k] + value
                pass_own(s + 1, k, True)

        @pl.when(jnp.logical_not(own))
        def _():
            for k in range(chunks):
                ybuf[s, c, k] = scaled(s, k)
                if not first:
                    to_column(s, k, owner).wait_send()
                to_column(s, k, owner).start()

        for k in range(chunks):
            swap(s, k).wait_send()

    multiply(0, True)
    reduce(0, True)

    def middle(s, carry):
        multiply(s, False)
        reduce(s, False)
        return carry

    lax.fori_loop(1, TERMS - 1, middle, 0)

    last = TERMS - 1
    multiply(last, False)
    for k in range(chunks):
        swap(last, k).start()
    for k in range(chunks):
        ybuf[last, c, k] = scaled(last, k) + run[k]

        @pl.when(jnp.logical_not(own))
        def _(k=k):
            to_column(last, k, owner).wait_send()

        for offset in range(1, cols):
            to_column(last, k, (c + offset) % cols).start()

    def give(k):
        part = pl.ds(pl.multiple_of((1 - p) * share, share), share)
        return remote(fin.at[k, part, :], frecv.at[k], f_send.at[k], f_recv.at[k], rep=1 - p)

    for k in range(chunks):
        fin[k] = column_sum(last, k)
        give(k).start()
        start = pl.multiple_of(p * half + k * TILE, TILE)
        out_ref[:, pl.ds(start, TILE)] = fin[k, pl.ds(pl.multiple_of(p * share, share), share), :]
    for k in range(chunks):
        give(k).wait()
        start = pl.multiple_of((1 - p) * half + k * TILE, TILE)
        out_ref[:, pl.ds(start, TILE)] = frecv[k]

    for k in range(chunks):
        swap(last, k).wait_send()
        for offset in range(1, cols):
            to_column(last, k, (c + offset) % cols).wait_send()

    def drain(step, carry):
        line, lane, j = block_of(step % fanout)
        for needed, copy in hops(last, first_line + line, lane, j, step // fanout):
            @pl.when(needed)
            def _(copy=copy):
                copy.wait_send()
        return carry

    lax.fori_loop(0, total, drain, 0)


def solution(mesh):
    rows, cols, reps = (mesh.shape[axis] for axis in ("row", "col", "rep"))

    def local(matrix, vectors):
        size, width = matrix.shape
        share = vectors.shape[0]
        every = share * reps
        fanout = rows // cols
        chunks = size // 2 // TILE
        tiles = size // TILE
        piece = (every, TILE)
        dma = pltpu.SemaphoreType.DMA
        return pl.pallas_call(
            functools.partial(kernel, rows, cols),
            out_shape=jax.ShapeDtypeStruct(vectors.shape, jnp.float32),
            in_specs=[pl.BlockSpec(memory_space=pltpu.HBM), pl.BlockSpec(memory_space=pltpu.VMEM)],
            out_specs=pl.BlockSpec(memory_space=pltpu.VMEM),
            scratch_shapes=[
                pltpu.VMEM((fanout * chunks, tiles, TILE, TILE), jnp.bfloat16),
                pltpu.VMEM((fanout * chunks, tiles, TILE, TILE), jnp.bfloat16),
                pltpu.VMEM((SLOTS, size, TILE), jnp.float32),
                pltpu.VMEM((TERMS, fanout, chunks) + piece, jnp.float32),
                pltpu.VMEM((tiles,) + piece, jnp.float32),
                pltpu.VMEM((TERMS, chunks) + piece, jnp.float32),
                pltpu.VMEM((TERMS, cols, chunks) + piece, jnp.float32),
                pltpu.VMEM((chunks,) + piece, jnp.float32),
                pltpu.VMEM((chunks,) + piece, jnp.float32),
                pltpu.VMEM((chunks, share, TILE), jnp.float32),
                dma((SLOTS,)),
                dma((chunks,)),
                dma((chunks,)),
                dma((2, fanout, chunks)),
                dma((fanout, chunks)),
                dma((fanout, chunks)),
                dma((fanout, chunks)),
                dma((chunks,)),
                dma((2, chunks)),
                dma((cols, chunks)),
                dma((2, cols, chunks)),
                dma((chunks,)),
                dma((chunks,)),
            ],
            compiler_params=pltpu.CompilerParams(
                collective_id=0, has_side_effects=True, vmem_limit_bytes=63 * 1024 * 1024
            ),
        )(matrix, vectors)

    return jax.shard_map(
        local, mesh=mesh, in_specs=(P("row", "col"), P("rep", "row")), out_specs=P("rep", "row"), check_vma=False
    )
```

```python
import functools

import jax
import jax.numpy as jnp
from jax import lax
from jax.experimental import pallas as pl
from jax.experimental.pallas import tpu as pltpu
from jax.sharding import PartitionSpec as P

TERMS = 6
STEPS = 1
MESH = pl.DeviceIdType.MESH
TILE = 256
SLOTS = 4
LAG = 4


def kernel(
    rows, cols, m_ref, v_ref, out_ref,
    high, low, stage, xbuf, acc, drecv, ybuf, run, fin, frecv,
    stage_sem, init_send, init_recv, x_recv, up_send, down_send, pair_send,
    d_send, d_recv, y_send, y_recv, f_send, f_recv,
):
    fanout = rows // cols
    size = m_ref.shape[0]
    share = v_ref.shape[0]
    half = size // 2
    chunks = half // TILE
    tiles = size // TILE
    lines = rows // 2
    depth = fanout // 2
    total = fanout * chunks

    r, c, p = lax.axis_index("row"), lax.axis_index("col"), lax.axis_index("rep")
    z, x = r // 2, r % 2
    first_line = c * depth
    owner = r // fanout
    own = owner == c
    mine = r % fanout

    barrier = pltpu.get_barrier_semaphore()

    def greet(**where):
        pl.semaphore_signal(barrier, inc=1, device_id=where, device_id_type=MESH)

    greet(rep=1 - p)
    greet(row=z * 2 + 1 - x)
    for offset in range(1, cols):
        greet(col=(c + offset) % cols)

    @pl.when(z > 0)
    def _():
        greet(row=r - 2)

    @pl.when(z < lines - 1)
    def _():
        greet(row=r + 2)

    def chunk_of(step):
        count = total // 2
        lag = min(LAG, count)
        mixed = step - lag
        alternate = jnp.where(mixed % 2 == 0, count + mixed // 2, lag + mixed // 2)
        place = jnp.where(step < lag, step, jnp.where(step < 2 * count - lag, alternate, step))
        other, place = place // count, place % count
        near = place // chunks
        line = jnp.where(z > first_line, depth - 1 - near, near)
        lane = jnp.where(other == 0, x, 1 - x)
        return line, lane, line * 2 + lane, place % chunks

    def load(step):
        _, _, j, k = chunk_of(step)
        start = pl.multiple_of(j * size + p * half + k * TILE, TILE)
        return pltpu.make_async_copy(
            m_ref.at[:, pl.ds(start, TILE)], stage.at[step % SLOTS], stage_sem.at[step % SLOTS]
        )

    for step in range(min(SLOTS, total)):
        load(step).start()

    pl.semaphore_wait(barrier, 1 + cols + (z > 0).astype(jnp.int32) + (z < lines - 1).astype(jnp.int32))

    def remote(source, target, send, recv, **where):
        return pltpu.make_async_remote_copy(
            src_ref=source, dst_ref=target, send_sem=send, recv_sem=recv,
            device_id=where, device_id_type=MESH,
        )

    def hops(s, line, lane, j, k):
        ref, recv = xbuf.at[s, j, k], x_recv.at[s % 2, j, k]
        here = lane == x
        return (
            (here & (z >= line) & (z < lines - 1), remote(ref, ref, up_send.at[j, k], recv, row=r + 2)),
            (here & (z <= line) & (z > 0), remote(ref, ref, down_send.at[j, k], recv, row=r - 2)),
            (here, remote(ref, ref, pair_send.at[j, k], recv, row=z * 2 + 1 - x)),
        )

    def pass_on(s, line, lane, j, k, again):
        for needed, copy in hops(s, line, lane, j, k):
            @pl.when(needed)
            def _(copy=copy):
                if again:
                    copy.wait_send()
                copy.start()

    def pass_own(s, k, again):
        pass_on(s, z, x, mine, k, again)

    @pl.when(own)
    def _():
        def given(k):
            start = pl.multiple_of((1 - p) * half + k * TILE, TILE)
            return remote(
                v_ref.at[:, pl.ds(start, TILE)],
                xbuf.at[0, mine, k, pl.ds(pl.multiple_of(p * share, share), share), :],
                init_send.at[k], init_recv.at[k], rep=1 - p,
            )

        for k in range(chunks):
            given(k).start()
        for k in range(chunks):
            start = pl.multiple_of(p * half + k * TILE, TILE)
            xbuf[0, mine, k, pl.ds(pl.multiple_of(p * share, share), share), :] = v_ref[:, pl.ds(start, TILE)]
        for k in range(chunks):
            given(k).wait()
            run[k] = xbuf[0, mine, k]
            pass_own(0, k, False)

    @pl.when(jnp.logical_not(own))
    def _():
        run[...] = jnp.zeros_like(run)

    def prepare(step, index):
        load(step).wait()
        for n in range(tiles):
            block = stage[step % SLOTS, n * TILE:(n + 1) * TILE, :]
            top = block.astype(jnp.bfloat16)
            rest = (block - top.astype(jnp.float32)).astype(jnp.bfloat16)
            high[index, n] = top.T
            low[index, n] = rest.T

        @pl.when(step + SLOTS < total)
        def _():
            load(step + SLOTS).start()

    def multiply(s, first):
        acc[...] = jnp.zeros_like(acc)

        def body(step, carry):
            line, lane, j, k = chunk_of(step)
            index = j * chunks + k
            if first:
                prepare(step, index)

            @pl.when(r != c * fanout + j)
            def _():
                remote(xbuf.at[s, j, k], xbuf.at[s, j, k], up_send.at[j, k], x_recv.at[s % 2, j, k], rep=1 - p).wait_recv()
                pass_on(s, first_line + line, lane, j, k, not first)

            value = xbuf[s, j, k]
            top = value.astype(jnp.bfloat16)
            rest = (value - top.astype(jnp.float32)).astype(jnp.bfloat16)
            both = jnp.concatenate([top, rest], axis=0)
            count = value.shape[0]
            for n in range(tiles):
                large = jnp.dot(both, high[index, n], preferred_element_type=jnp.float32)
                small = jnp.dot(top, low[index, n], preferred_element_type=jnp.float32)
                acc[n] += large[:count] + (large[count:] + small)
            return carry

        lax.fori_loop(0, total, body, 0)

    def swap(s, k):
        return remote(
            acc.at[(1 - p) * chunks + k], drecv.at[s, k], d_send.at[k], d_recv.at[s % 2, k], rep=1 - p
        )

    def to_column(s, k, target):
        return remote(
            ybuf.at[s, c, k], ybuf.at[s, c, k], y_send.at[target, k], y_recv.at[s % 2, c, k], col=target
        )

    def from_column(s, k, source):
        return remote(
            ybuf.at[s, source, k], ybuf.at[s, source, k], y_send.at[source, k], y_recv.at[s % 2, source, k], col=source
        )

    def column_sum(s, k):
        for offset in range(1, cols):
            from_column(s, k, (c + offset) % cols).wait_recv()
        value = ybuf[s, 0, k]
        for source in range(1, cols):
            value = value + ybuf[s, source, k]
        return value

    def scaled(s, k):
        swap(s, k).wait_recv()
        degree = jnp.asarray((s + 1) * STEPS, jnp.int32).astype(jnp.float32)
        return (acc[p * chunks + k] + drecv[s, k]) / degree

    def reduce(s, first):
        for k in range(chunks):
            swap(s, k).start()

        @pl.when(own)
        def _():
            for k in range(chunks):
                ybuf[s, c, k] = scaled(s, k)
                value = column_sum(s, k)
                xbuf[s + 1, mine, k] = value
                run[k] = run[k] + value
                pass_own(s + 1, k, True)

        @pl.when(jnp.logical_not(own))
        def _():
            for k in range(chunks):
                ybuf[s, c, k] = scaled(s, k)
                if not first:
                    to_column(s, k, owner).wait_send()
                to_column(s, k, owner).start()

        for k in range(chunks):
            swap(s, k).wait_send()

    multiply(0, True)
    reduce(0, True)

    def middle(s, carry):
        multiply(s, False)
        reduce(s, False)
        return carry

    lax.fori_loop(1, TERMS - 1, middle, 0)

    last = TERMS - 1
    multiply(last, False)
    for k in range(chunks):
        swap(last, k).start()
    for k in range(chunks):
        ybuf[last, c, k] = scaled(last, k) + run[k]

        @pl.when(jnp.logical_not(own))
        def _(k=k):
            to_column(last, k, owner).wait_send()

        for offset in range(1, cols):
            to_column(last, k, (c + offset) % cols).start()

    def give(k):
        part = pl.ds(pl.multiple_of((1 - p) * share, share), share)
        return remote(fin.at[k, part, :], frecv.at[k], f_send.at[k], f_recv.at[k], rep=1 - p)

    for k in range(chunks):
        fin[k] = column_sum(last, k)
        give(k).start()
        start = pl.multiple_of(p * half + k * TILE, TILE)
        out_ref[:, pl.ds(start, TILE)] = fin[k, pl.ds(pl.multiple_of(p * share, share), share), :]
    for k in range(chunks):
        give(k).wait()
        start = pl.multiple_of((1 - p) * half + k * TILE, TILE)
        out_ref[:, pl.ds(start, TILE)] = frecv[k]

    for k in range(chunks):
        swap(last, k).wait_send()
        for offset in range(1, cols):
            to_column(last, k, (c + offset) % cols).wait_send()

    def drain(step, carry):
        line, lane, j, k = chunk_of(step)
        for needed, copy in hops(last, first_line + line, lane, j, k):
            @pl.when(needed)
            def _(copy=copy):
                copy.wait_send()
        return carry

    lax.fori_loop(0, total, drain, 0)


def solution(mesh):
    rows, cols, reps = (mesh.shape[axis] for axis in ("row", "col", "rep"))

    def local(matrix, vectors):
        size, width = matrix.shape
        share = vectors.shape[0]
        every = share * reps
        fanout = rows // cols
        chunks = size // 2 // TILE
        tiles = size // TILE
        piece = (every, TILE)
        dma = pltpu.SemaphoreType.DMA
        return pl.pallas_call(
            functools.partial(kernel, rows, cols),
            out_shape=jax.ShapeDtypeStruct(vectors.shape, jnp.float32),
            in_specs=[pl.BlockSpec(memory_space=pltpu.HBM), pl.BlockSpec(memory_space=pltpu.VMEM)],
            out_specs=pl.BlockSpec(memory_space=pltpu.VMEM),
            scratch_shapes=[
                pltpu.VMEM((fanout * chunks, tiles, TILE, TILE), jnp.bfloat16),
                pltpu.VMEM((fanout * chunks, tiles, TILE, TILE), jnp.bfloat16),
                pltpu.VMEM((SLOTS, size, TILE), jnp.float32),
                pltpu.VMEM((TERMS, fanout, chunks) + piece, jnp.float32),
                pltpu.VMEM((tiles,) + piece, jnp.float32),
                pltpu.VMEM((TERMS, chunks) + piece, jnp.float32),
                pltpu.VMEM((TERMS, cols, chunks) + piece, jnp.float32),
                pltpu.VMEM((chunks,) + piece, jnp.float32),
                pltpu.VMEM((chunks,) + piece, jnp.float32),
                pltpu.VMEM((chunks, share, TILE), jnp.float32),
                dma((SLOTS,)),
                dma((chunks,)),
                dma((chunks,)),
                dma((2, fanout, chunks)),
                dma((fanout, chunks)),
                dma((fanout, chunks)),
                dma((fanout, chunks)),
                dma((chunks,)),
                dma((2, chunks)),
                dma((cols, chunks)),
                dma((2, cols, chunks)),
                dma((chunks,)),
                dma((chunks,)),
            ],
            compiler_params=pltpu.CompilerParams(
                collective_id=0, has_side_effects=True, vmem_limit_bytes=63 * 1024 * 1024
            ),
        )(matrix, vectors)

    return jax.shard_map(
        local, mesh=mesh, in_specs=(P("row", "col"), P("rep", "row")), out_specs=P("rep", "row"), check_vma=False
    )
```

```python
import functools

import jax
import jax.numpy as jnp
from jax import lax
from jax.experimental import pallas as pl
from jax.experimental.pallas import tpu as pltpu
from jax.sharding import PartitionSpec as P

TERMS = 6
STEPS = 1
MESH = pl.DeviceIdType.MESH
TILE = 256
SLOTS = 4
LAG = 5
SPLIT = 2


def kernel(
    rows, cols, m_ref, v_ref, out_ref,
    high, low, stage, xbuf, acc, drecv, ybuf, run, fin, frecv,
    stage_sem, init_send, init_recv, x_recv, up_send, down_send, pair_send,
    d_send, d_recv, y_send, y_recv, f_send, f_recv,
):
    fanout = rows // cols
    size = m_ref.shape[0]
    share = v_ref.shape[0]
    half = size // 2
    chunks = half // TILE
    tiles = size // TILE
    lines = rows // 2
    depth = fanout // 2
    total = fanout * chunks

    r, c, p = lax.axis_index("row"), lax.axis_index("col"), lax.axis_index("rep")
    z, x = r // 2, r % 2
    first_line = c * depth
    owner = r // fanout
    own = owner == c
    mine = r % fanout

    barrier = pltpu.get_barrier_semaphore()

    def greet(**where):
        pl.semaphore_signal(barrier, inc=1, device_id=where, device_id_type=MESH)

    greet(rep=1 - p)
    greet(row=z * 2 + 1 - x)
    for offset in range(1, cols):
        greet(col=(c + offset) % cols)

    @pl.when(z > 0)
    def _():
        greet(row=r - 2)

    @pl.when(z < lines - 1)
    def _():
        greet(row=r + 2)

    def chunk_of(step):
        count = total // 2
        lag = min(LAG, count)
        mixed = step - lag
        alternate = jnp.where(mixed % 2 == 0, count + mixed // 2, lag + mixed // 2)
        place = jnp.where(step < lag, step, jnp.where(step < 2 * count - lag, alternate, step))
        other, place = place // count, place % count
        near = place // chunks
        line = jnp.where(z > first_line, depth - 1 - near, near)
        lane = jnp.where(other == 0, x, 1 - x)
        return line, lane, line * 2 + lane, place % chunks

    def load(step):
        _, _, j, k = chunk_of(step)
        start = pl.multiple_of(j * size + p * half + k * TILE, TILE)
        return pltpu.make_async_copy(
            m_ref.at[:, pl.ds(start, TILE)], stage.at[step % SLOTS], stage_sem.at[step % SLOTS]
        )

    for step in range(min(SLOTS, total)):
        load(step).start()

    pl.semaphore_wait(barrier, 1 + cols + (z > 0).astype(jnp.int32) + (z < lines - 1).astype(jnp.int32))

    def remote(source, target, send, recv, **where):
        return pltpu.make_async_remote_copy(
            src_ref=source, dst_ref=target, send_sem=send, recv_sem=recv,
            device_id=where, device_id_type=MESH,
        )

    part = share * 2 // SPLIT

    def hops(s, line, lane, j, k, h):
        ref, recv = xbuf.at[s, j, k, pl.ds(h * part, part), :], x_recv.at[s % 2, j, k, h]
        here = lane == x
        return (
            (here & (z >= line) & (z < lines - 1), remote(ref, ref, up_send.at[j, k, h], recv, row=r + 2)),
            (here & (z <= line) & (z > 0), remote(ref, ref, down_send.at[j, k, h], recv, row=r - 2)),
            (here, remote(ref, ref, pair_send.at[j, k, h], recv, row=z * 2 + 1 - x)),
        )

    def pass_on(s, line, lane, j, k, h, again):
        for needed, copy in hops(s, line, lane, j, k, h):
            @pl.when(needed)
            def _(copy=copy):
                if again:
                    copy.wait_send()
                copy.start()

    def pass_own(s, k, h, again):
        pass_on(s, z, x, mine, k, h, again)

    @pl.when(own)
    def _():
        def given(k):
            start = pl.multiple_of((1 - p) * half + k * TILE, TILE)
            return remote(
                v_ref.at[:, pl.ds(start, TILE)],
                xbuf.at[0, mine, k, pl.ds(pl.multiple_of(p * share, share), share), :],
                init_send.at[k], init_recv.at[k], rep=1 - p,
            )

        for k in range(chunks):
            given(k).start()
        for k in range(chunks):
            start = pl.multiple_of(p * half + k * TILE, TILE)
            xbuf[0, mine, k, pl.ds(pl.multiple_of(p * share, share), share), :] = v_ref[:, pl.ds(start, TILE)]
        for k in range(chunks):
            given(k).wait()
            run[k] = xbuf[0, mine, k]
            for h in range(SPLIT):
                pass_own(0, k, h, False)

    @pl.when(jnp.logical_not(own))
    def _():
        run[...] = jnp.zeros_like(run)

    def prepare(step, index):
        load(step).wait()
        for n in range(tiles):
            block = stage[step % SLOTS, n * TILE:(n + 1) * TILE, :]
            top = block.astype(jnp.bfloat16)
            rest = (block - top.astype(jnp.float32)).astype(jnp.bfloat16)
            high[index, n] = top.T
            low[index, n] = rest.T

        @pl.when(step + SLOTS < total)
        def _():
            load(step + SLOTS).start()

    def multiply(s, first):
        acc[...] = jnp.zeros_like(acc)

        def body(step, carry):
            line, lane, j, k = chunk_of(step)
            index = j * chunks + k
            if first:
                prepare(step, index)

            @pl.when(r != c * fanout + j)
            def _():
                for h in range(SPLIT):
                    ref = xbuf.at[s, j, k, pl.ds(h * part, part), :]
                    remote(ref, ref, up_send.at[j, k, h], x_recv.at[s % 2, j, k, h], rep=1 - p).wait_recv()
                    pass_on(s, first_line + line, lane, j, k, h, not first)

            value = xbuf[s, j, k]
            top = value.astype(jnp.bfloat16)
            rest = (value - top.astype(jnp.float32)).astype(jnp.bfloat16)
            both = jnp.concatenate([top, rest], axis=0)
            count = value.shape[0]
            for n in range(tiles):
                large = jnp.dot(both, high[index, n], preferred_element_type=jnp.float32)
                small = jnp.dot(top, low[index, n], preferred_element_type=jnp.float32)
                acc[n] += large[:count] + (large[count:] + small)
            return carry

        lax.fori_loop(0, total, body, 0)

    def swap(s, k):
        return remote(
            acc.at[(1 - p) * chunks + k], drecv.at[s, k], d_send.at[k], d_recv.at[s % 2, k], rep=1 - p
        )

    def to_column(s, k, h, target):
        ref = ybuf.at[s, c, k, pl.ds(h * part, part), :]
        return remote(ref, ref, y_send.at[target, k, h], y_recv.at[s % 2, c, k, h], col=target)

    def from_column(s, k, h, source):
        ref = ybuf.at[s, source, k, pl.ds(h * part, part), :]
        return remote(ref, ref, y_send.at[source, k, h], y_recv.at[s % 2, source, k, h], col=source)

    def column_sum(s, k, h):
        for offset in range(1, cols):
            from_column(s, k, h, (c + offset) % cols).wait_recv()
        value = ybuf[s, 0, k, h * part:(h + 1) * part, :]
        for source in range(1, cols):
            value = value + ybuf[s, source, k, h * part:(h + 1) * part, :]
        return value

    def scaled(s, k):
        swap(s, k).wait_recv()
        degree = jnp.asarray((s + 1) * STEPS, jnp.int32).astype(jnp.float32)
        return (acc[p * chunks + k] + drecv[s, k]) / degree

    def reduce(s, first):
        for k in range(chunks):
            swap(s, k).start()

        @pl.when(own)
        def _():
            for k in range(chunks):
                ybuf[s, c, k] = scaled(s, k)
                for h in range(SPLIT):
                    piece = slice(h * part, (h + 1) * part)
                    value = column_sum(s, k, h)
                    xbuf[s + 1, mine, k, piece, :] = value
                    run[k, piece, :] = run[k, piece, :] + value
                    pass_own(s + 1, k, h, True)

        @pl.when(jnp.logical_not(own))
        def _():
            for k in range(chunks):
                ybuf[s, c, k] = scaled(s, k)
                for h in range(SPLIT):
                    if not first:
                        to_column(s, k, h, owner).wait_send()
                    to_column(s, k, h, owner).start()

        for k in range(chunks):
            swap(s, k).wait_send()

    multiply(0, True)
    reduce(0, True)

    def middle(s, carry):
        multiply(s, False)
        reduce(s, False)
        return carry

    lax.fori_loop(1, TERMS - 1, middle, 0)

    last = TERMS - 1
    multiply(last, False)
    for k in range(chunks):
        swap(last, k).start()
    for k in range(chunks):
        ybuf[last, c, k] = scaled(last, k) + run[k]

        @pl.when(jnp.logical_not(own))
        def _(k=k):
            for h in range(SPLIT):
                to_column(last, k, h, owner).wait_send()

        for offset in range(1, cols):
            for h in range(SPLIT):
                to_column(last, k, h, (c + offset) % cols).start()

    def give(k):
        theirs = pl.ds(pl.multiple_of((1 - p) * share, share), share)
        return remote(fin.at[k, theirs, :], frecv.at[k], f_send.at[k], f_recv.at[k], rep=1 - p)

    for k in range(chunks):
        for h in range(SPLIT):
            fin[k, h * part:(h + 1) * part, :] = column_sum(last, k, h)
        give(k).start()
        start = pl.multiple_of(p * half + k * TILE, TILE)
        out_ref[:, pl.ds(start, TILE)] = fin[k, pl.ds(pl.multiple_of(p * share, share), share), :]
    for k in range(chunks):
        give(k).wait()
        start = pl.multiple_of((1 - p) * half + k * TILE, TILE)
        out_ref[:, pl.ds(start, TILE)] = frecv[k]

    for k in range(chunks):
        swap(last, k).wait_send()
        for offset in range(1, cols):
            for h in range(SPLIT):
                to_column(last, k, h, (c + offset) % cols).wait_send()

    def drain(step, carry):
        line, lane, j, k = chunk_of(step)
        for h in range(SPLIT):
            for needed, copy in hops(last, first_line + line, lane, j, k, h):
                @pl.when(needed)
                def _(copy=copy):
                    copy.wait_send()
        return carry

    lax.fori_loop(0, total, drain, 0)


def solution(mesh):
    rows, cols, reps = (mesh.shape[axis] for axis in ("row", "col", "rep"))

    def local(matrix, vectors):
        size, width = matrix.shape
        share = vectors.shape[0]
        every = share * reps
        fanout = rows // cols
        chunks = size // 2 // TILE
        tiles = size // TILE
        piece = (every, TILE)
        dma = pltpu.SemaphoreType.DMA
        return pl.pallas_call(
            functools.partial(kernel, rows, cols),
            out_shape=jax.ShapeDtypeStruct(vectors.shape, jnp.float32),
            in_specs=[pl.BlockSpec(memory_space=pltpu.HBM), pl.BlockSpec(memory_space=pltpu.VMEM)],
            out_specs=pl.BlockSpec(memory_space=pltpu.VMEM),
            scratch_shapes=[
                pltpu.VMEM((fanout * chunks, tiles, TILE, TILE), jnp.bfloat16),
                pltpu.VMEM((fanout * chunks, tiles, TILE, TILE), jnp.bfloat16),
                pltpu.VMEM((SLOTS, size, TILE), jnp.float32),
                pltpu.VMEM((TERMS, fanout, chunks) + piece, jnp.float32),
                pltpu.VMEM((tiles,) + piece, jnp.float32),
                pltpu.VMEM((TERMS, chunks) + piece, jnp.float32),
                pltpu.VMEM((TERMS, cols, chunks) + piece, jnp.float32),
                pltpu.VMEM((chunks,) + piece, jnp.float32),
                pltpu.VMEM((chunks,) + piece, jnp.float32),
                pltpu.VMEM((chunks, share, TILE), jnp.float32),
                dma((SLOTS,)),
                dma((chunks,)),
                dma((chunks,)),
                dma((2, fanout, chunks, SPLIT)),
                dma((fanout, chunks, SPLIT)),
                dma((fanout, chunks, SPLIT)),
                dma((fanout, chunks, SPLIT)),
                dma((chunks,)),
                dma((2, chunks)),
                dma((cols, chunks, SPLIT)),
                dma((2, cols, chunks, SPLIT)),
                dma((chunks,)),
                dma((chunks,)),
            ],
            compiler_params=pltpu.CompilerParams(
                collective_id=0, has_side_effects=True, vmem_limit_bytes=63 * 1024 * 1024
            ),
        )(matrix, vectors)

    return jax.shard_map(
        local, mesh=mesh, in_specs=(P("row", "col"), P("rep", "row")), out_specs=P("rep", "row"), check_vma=False
    )
```
